256 devices in a mesh: rep: 2 (over core), dp: 128 (over x, y, z).
Axes of the slice: x: 4, y: 4, z: 8, core: 2. Of those that a mesh axis runs over, the one named last changes fastest.
Arguments:
- x: bfloat16 [256, 2048, 896], P(('rep', 'dp')), parts along dimension 0
- dy: bfloat16 [256, 2048, 896], P(('rep', 'dp')), parts along dimension 0
- w_gate: bfloat16 [2, 896, 2560], replicated
- w_up: bfloat16 [2, 896, 2560], replicated
- w_down: bfloat16 [2, 2560, 896], replicated
- m_w_gate: float32 [2, 896, 2560], P(None, 'dp')
- m_w_up: float32 [2, 896, 2560], P(None, 'dp')
- m_w_down: float32 [2, 2560, 896], P(None, 'dp')
- v_w_gate: float32 [2, 896, 2560], P(None, 'dp')
- v_w_up: float32 [2, 896, 2560], P(None, 'dp')
- v_w_down: float32 [2, 2560, 896], P(None, 'dp')
Outputs:
- output 1: bfloat16 [4, 896, 2560], P('rep'), parts along dimension 0
- output 2: bfloat16 [4, 896, 2560], P('rep'), parts along dimension 0
- output 3: bfloat16 [4, 2560, 896], P('rep'), parts along dimension 0
- output 4: float32 [4, 896, 2560], P('rep', 'dp'), parts along dimension 0
- output 5: float32 [4, 896, 2560], P('rep', 'dp'), parts along dimension 0
- output 6: float32 [4, 2560, 896], P('rep', 'dp'), parts along dimension 0
- output 7: float32 [4, 896, 2560], P('rep', 'dp'), parts along dimension 0
- output 8: float32 [4, 896, 2560], P('rep', 'dp'), parts along dimension 0
- output 9: float32 [4, 2560, 896], P('rep', 'dp'), parts along dimension 0
There are 2 independent parts. The reference program is written for one: setup_inputs(seed, part) draws one part's arguments, and reference() takes and returns one part's arrays. A program takes and returns all parts, laid end to end along the dimension named above; an argument that names none is the same for every part.
All inputs are finite; a program needn't handle non-finite values.
Results may differ from the reference program's by a relative error of at most 0.022.
Values are sent between devices in bfloat16 or wider.
A program may use at most 768 MiB of HBM per device.

```python
import jax
import jax.numpy as jnp
from jax import lax

SEQUENCES = 128
TOKENS = 2048
D = 896
FF = 2560
LAYERS = 2
NAMES = ("w_gate", "w_up", "w_down")
SHAPES = {"w_gate": (LAYERS, D, FF), "w_up": (LAYERS, D, FF), "w_down": (LAYERS, FF, D)}


def bump(key, n, height):
    away = (jnp.arange(n, dtype=jnp.int32) - jax.random.randint(key, (), 0, n, jnp.int32)) % n
    return jnp.where(away < n // 8, height, 1.0)


def together(key, own, strength):
    shared = jax.random.normal(key, own.shape[1:], jnp.float32)
    return (own + strength * shared) * lax.rsqrt(1 + strength * strength)


def setup_inputs(seed: int = 0, part: int = 0) -> dict:
    kx, kdy, ka, kb, kz, kf, kh, kl, *keys = jax.random.split(jax.random.key(seed), 8 + 3 * len(NAMES))
    kx, kdy, ka, kb = (jax.random.fold_in(k, part) for k in (kx, kdy, ka, kb))
    kw, km, kv = (keys[i::3] for i in range(3))
    shape = (SEQUENCES, TOKENS, D)
    much_x, much_dy = jax.random.uniform(kz, (2,), jnp.float32, 0.0, 1.0)
    loud = 2.0 ** jax.random.uniform(jax.random.fold_in(kz, 1), (), jnp.float32, -1.0, 2.0)
    layers = 2.0 ** jax.random.uniform(kl, (LAYERS, 1, 1), jnp.float32, -1.0, 1.0)
    x = together(ka, jax.random.normal(kx, shape, jnp.float32), much_x) * bump(kf, D, 4.0)
    dy = together(kb, jax.random.normal(kdy, shape, jnp.float32), much_dy)
    drawn = {"x": x.astype(jnp.bfloat16), "dy": (loud * dy * (SEQUENCES * TOKENS) ** -0.5).astype(jnp.bfloat16)}
    for key, name in zip(kw, NAMES, strict=True):
        w = jax.random.normal(key, SHAPES[name], jnp.float32) * SHAPES[name][1] ** -0.5
        drawn[name] = (w * {"w_gate": 1.0, "w_up": bump(kh, FF, 4.0), "w_down": layers}[name]).astype(jnp.bfloat16)
    for key, name in zip(km, NAMES, strict=True):
        drawn[f"m_{name}"] = 0.1 * jax.random.normal(key, SHAPES[name], jnp.float32)
    for key, name in zip(kv, NAMES, strict=True):
        drawn[f"v_{name}"] = loud * loud * jax.random.uniform(key, SHAPES[name], jnp.float32, 0.05, 0.15)
    return drawn


def matmul(a, w):
    return jnp.dot(a, w, preferred_element_type=jnp.float32).astype(jnp.bfloat16)


def normed(h):
    wide = h.astype(jnp.float32)
    scale = lax.rsqrt(jnp.mean(wide**2, -1, keepdims=True) + 1e-6)
    return (wide * scale).astype(jnp.bfloat16)


def layer(h, w):
    a = normed(h)
    gate = jnp.dot(a, w["w_gate"], preferred_element_type=jnp.float32)
    up = jnp.dot(a, w["w_up"], preferred_element_type=jnp.float32)
    return h + matmul((jax.nn.silu(gate) * up).astype(jnp.bfloat16), w["w_down"])


def adamw(w, m, v, g):
    m = 0.9 * m + 0.1 * g
    v = 0.95 * v + 0.05 * g * g
    step = m * lax.rsqrt(v + 1e-8) + 0.1 * w
    return (w - 0.02 * step).astype(jnp.bfloat16), m, v


def stack(weights, h):
    return lax.scan(lambda h, w: (layer(h, w), None), h, weights)[0]


def reference(x, dy, w_gate, w_up, w_down, m_w_gate, m_w_up, m_w_down, v_w_gate, v_w_up, v_w_down):
    weights = dict(zip(NAMES, (w_gate, w_up, w_down), strict=True))

    def take(so_far, sequence):
        h, by_y = sequence
        _, back = jax.vjp(lambda w: stack(w, h), weights)
        return jax.tree.map(lambda total, term: total + term.astype(jnp.float32), so_far, back(by_y)[0]), None

    none_yet = {name: jnp.zeros(w.shape, jnp.float32) for name, w in weights.items()}
    by_weights, _ = lax.scan(take, none_yet, (x, dy))
    gradients = [by_weights[name].astype(jnp.bfloat16).astype(jnp.float32) for name in NAMES]
    new = [
        adamw(w.astype(jnp.float32), m, v, g)
        for w, m, v, g in zip((w_gate, w_up, w_down), (m_w_gate, m_w_up, m_w_down), (v_w_gate, v_w_up, v_w_down), gradients, strict=True)
    ]
    return tuple(one[which] for which in range(3) for one in new)
```

```python
import functools

import jax
import jax.numpy as jnp
from jax import lax
from jax.experimental import pallas as pl
from jax.experimental.pallas import tpu as pltpu
from jax.sharding import PartitionSpec as P

NX, NY, NZ = 4, 4, 8
D, FF = 896, 2560
F32, BF16 = jnp.float32, jnp.bfloat16

GATE = dict(r=7, rp=8, widths=(640, 640, 1280))
UP = dict(r=7, rp=8, widths=(768, 768, 1024))
DOWN1 = dict(r=20, rp=24, widths=(512, 384, 0))
DOWN0 = dict(r=20, rp=24, widths=(384, 512, 0))
CHUNKS = (
    ("w_down", 1, DOWN1, 1, "x"),
    ("w_gate", 1, GATE, -1, "x"),
    ("w_up", 1, UP, 1, "y"),
    ("w_down", 0, DOWN0, -1, "x"),
    ("w_gate", 0, GATE, 1, "x"),
    ("w_up", 0, UP, -1, "y"),
)


class Torus:
    def __init__(self):
        self.size = {"x": NX, "y": NY, "z": NZ}
        dp = lax.axis_index("dp")
        self.rep = lax.axis_index("rep")
        self.me = {"x": dp // (NY * NZ), "y": lax.rem(dp // NZ, NY), "z": lax.rem(dp, NZ)}

    def shifted(self, axis, by):
        return lax.rem(self.me[axis] + by + self.size[axis], self.size[axis])

    def neighbour(self, axis, by):
        place = dict(self.me)
        place[axis] = self.shifted(axis, by)
        return (self.rep, (place["x"] * NY + place["y"]) * NZ + place["z"])

    def barrier(self):
        sem = pltpu.get_barrier_semaphore()
        count = 0
        for axis in "xyz":
            for by in (1, -1):
                if self.size[axis] > (1 if by == 1 else 2):
                    pl.semaphore_signal(sem, inc=1, device_id=self.neighbour(axis, by), device_id_type=pl.DeviceIdType.MESH)
                    count += 1
        pl.semaphore_wait(sem, count)


class Ring:
    def __init__(self, torus, axis, sign, send, recv, base):
        n = torus.size[axis]
        self.torus, self.axis, self.n = torus, axis, n
        self.signs = (sign, -sign)
        self.hops = (n // 2, n - 1 - n // 2)
        self.send, self.recv, self.base = send, recv, base
        self.started = []

    def slot(self, flow, hop):
        return hop - 1 + (self.hops[0] if flow else 0)

    def copy(self, flow, hop, src, dst):
        at = self.base + self.slot(flow, hop)
        return pltpu.make_async_remote_copy(
            src_ref=src,
            dst_ref=dst,
            send_sem=self.send.at[at],
            recv_sem=self.recv.at[at],
            device_id=self.torus.neighbour(self.axis, self.signs[flow]),
            device_id_type=pl.DeviceIdType.MESH,
        )

    def start(self, flow, hop, src, dst):
        copy = self.copy(flow, hop, src, dst)
        copy.start()
        self.started.append(copy)

    def drain(self):
        for copy in self.started:
            copy.wait_send()


def total(into, terms):
    *lead, rows, columns = into.shape
    block = max(b for b in range(8, rows + 1, 8) if rows % b == 0 and (b == 8 or b * columns <= 40 * 1024))
    per = rows // block
    count = per
    for n in lead:
        count *= n

    def step(i, carry):
        at = []
        if per > 1:
            at = [pl.ds(pl.multiple_of(lax.rem(i, per) * block, block), block)]
            i = i // per
        else:
            at = [slice(None)]
        for n in reversed(lead):
            at.insert(0, lax.rem(i, n))
            i = i // n
        at = tuple(at)
        value = terms[0][at].astype(F32)
        for term in terms[1:]:
            value = value + term[at].astype(F32)
        into[at] = value.astype(into.dtype)
        return carry

    if count == 1:
        step(0, 0)
    else:
        lax.fori_loop(0, count, step, 0)


class SumOver:
    def __init__(self, ring, piece, terms, got):
        self.ring, self.piece, self.terms, self.got = ring, piece, terms, got

    def shard(self, flow, hop):
        return self.ring.torus.shifted(self.ring.axis, self.ring.signs[flow] * (self.ring.hops[flow] - hop))

    def pass_on(self, flow, hop):
        ring = self.ring
        if hop >= ring.hops[flow]:
            return
        i = self.shard(flow, hop)
        piece, terms = self.piece(i), list(self.terms(i))
        if hop:
            got = self.got.at[ring.slot(flow, hop)]
            ring.copy(flow, hop, got, got).wait_recv()
            terms.append(got)
        if len(terms) > 1 or terms[0] is not piece:
            total(piece, terms)
        ring.start(flow, hop + 1, piece, self.got.at[ring.slot(flow, hop + 1)])

    def step(self, hop):
        for flow in (0, 1):
            self.pass_on(flow, hop)

    def arrived(self):
        slots = []
        for flow in (0, 1):
            if self.ring.hops[flow]:
                slot = self.ring.slot(flow, self.ring.hops[flow])
                self.ring.copy(flow, self.ring.hops[flow], self.got.at[slot], self.got.at[slot]).wait_recv()
                slots.append(slot)
        return slots


def sums_xy(torus, first, second, own, got, wide, pieces, out, sign, sems, r, rp):
    me = torus.me
    flat, padded = wide
    send, recv, base = sems
    n1, n2 = torus.size[first], torus.size[second]
    rings = (
        Ring(torus, first, sign, send, recv, base),
        Ring(torus, second, sign, send, recv, base + n1 - 1),
        Ring(torus, "z", sign, send, recv, base + n1 + n2 - 2),
    )
    if first == "x":
        of_first, of_both = (lambda i: own.at[i]), (lambda j: own.at[me["x"], j])
    else:
        of_first, of_both = (lambda i: own.at[:, i]), (lambda j: own.at[j, me["y"]])
    one = SumOver(rings[0], of_first, lambda i: [of_first(i)], got[0])
    one.terms = None
    state = {}

    def first_pass(hop):
        for flow in (0, 1):
            if hop >= rings[0].hops[flow]:
                continue
            i = one.shard(flow, hop)
            piece = of_first(i)
            if hop:
                arrived = got[0].at[rings[0].slot(flow, hop)]
                rings[0].copy(flow, hop, arrived, arrived).wait_recv()
                total(piece, [piece, arrived])
            rings[0].start(flow, hop + 1, piece, got[0].at[rings[0].slot(flow, hop + 1)])

    def second_start():
        slots = one.arrived()
        terms = lambda j: [of_both(j)] + [got[0].at[s, j] for s in slots]
        state["two"] = SumOver(rings[1], of_both, terms, got[1])
        state["terms"] = terms
        state["two"].step(0)

    def third_start():
        slots = state["two"].arrived()
        total(flat, state["terms"](me[second]) + [got[1].at[s] for s in slots])
        for z in range(NZ):
            padded[z, 0:r, :] = flat[z * r : (z + 1) * r, :]
        state["three"] = SumOver(rings[2], lambda k: pieces.at[k], lambda k: [padded.at[k]], got[2])
        state["three"].step(0)

    def finish():
        slots = state["three"].arrived()
        total(out, [padded.at[me["z"]]] + [got[2].at[s] for s in slots])
        for ring in rings:
            ring.drain()

    stages = [functools.partial(first_pass, h) for h in range(max(1, n1 // 2))]
    stages.append(second_start)
    stages += [functools.partial(lambda h: state["two"].step(h), h) for h in range(1, n2 // 2)]
    stages.append(third_start)
    stages += [functools.partial(lambda h: state["three"].step(h), h) for h in range(1, NZ // 2)]
    stages.append(finish)
    return stages


def sums_z(torus, second, own, got, out, sign, sems):
    me = torus.me
    third = "y" if second == "x" else "x"
    send, recv, base = sems
    n2, n3 = torus.size[second], torus.size[third]
    rings = (
        Ring(torus, "z", sign, send, recv, base),
        Ring(torus, second, sign, send, recv, base + NZ - 1),
        Ring(torus, third, sign, send, recv, base + NZ + n2 - 2),
    )
    of_one = lambda k: own.at[:, :, k]
    if second == "x":
        own_two, got_two = (lambda i: own.at[i, :, me["z"]]), (lambda s, i: got[0].at[s, i])
        own_three = lambda j: own.at[me["x"], j, me["z"]]
        got_three = lambda s, j: got[0].at[s, me["x"], j]
    else:
        own_two, got_two = (lambda j: own.at[:, j, me["z"]]), (lambda s, j: got[0].at[s, :, j])
        own_three = lambda i: own.at[i, me["y"], me["z"]]
        got_three = lambda s, i: got[0].at[s, i, me["y"]]
    one = SumOver(rings[0], None, None, got[0])
    state = {}

    def first_pass(hop):
        for flow in (0, 1):
            if hop >= rings[0].hops[flow]:
                continue
            piece = of_one(one.shard(flow, hop))
            if hop:
                arrived = got[0].at[rings[0].slot(flow, hop)]
                rings[0].copy(flow, hop, arrived, arrived).wait_recv()
                total(piece, [piece, arrived])
            rings[0].start(flow, hop + 1, piece, got[0].at[rings[0].slot(flow, hop + 1)])

    def second_start():
        state["one"] = one.arrived()
        terms = lambda i: [own_two(i)] + [got_two(s, i) for s in state["one"]]
        state["two"] = SumOver(rings[1], own_two, terms, got[1])
        state["two"].step(0)

    def third_start():
        slots = state["two"].arrived()
        terms = lambda j: [own_three(j)] + [got_three(s, j) for s in state["one"]] + [got[1].at[s, j] for s in slots]
        state["terms"] = terms
        state["three"] = SumOver(rings[2], own_three, terms, got[2])
        state["three"].step(0)

    def finish():
        slots = state["three"].arrived()
        total(out, state["terms"](me[third]) + [got[2].at[s] for s in slots])
        for ring in rings:
            ring.drain()

    stages = [functools.partial(first_pass, h) for h in range(max(1, NZ // 2))]
    stages.append(second_start)
    stages += [functools.partial(lambda h: state["two"].step(h), h) for h in range(1, n2 // 2)]
    stages.append(third_start)
    stages += [functools.partial(lambda h: state["three"].step(h), h) for h in range(1, n3 // 2)]
    stages.append(finish)
    return stages


HOPS = (NX - 1) + (NY - 1) + (NZ - 1)


def own_shape(shape, kind):
    width = shape["widths"][kind]
    return (NX, NY, NZ, shape["rp"], width) if kind == 2 else (NX, NY, NZ * shape["r"], width)


def ranges():
    return [(c, kind) for c, chunk in enumerate(CHUNKS) for kind in range(3) if chunk[2]["widths"][kind]]


def run_in_slots(stages_of):
    slots = max(c + max(len(s) for s in stages) for c, stages in enumerate(stages_of))
    for slot in range(slots):
        for c in range(len(stages_of) - 1, -1, -1):
            for stages in stages_of[c]:
                if 0 <= slot - c < len(stages):
                    stages[slot - c]()


def reduce_kernel(*refs):
    todo = ranges()
    count = len(todo)
    ins, outs = refs[:count], refs[count : count + len(CHUNKS)]
    rest = list(refs[count + len(CHUNKS) :])
    load, send, recv = rest[:3]
    rest = rest[3:]
    torus = Torus()
    stages_of = [[] for _ in CHUNKS]
    loads = []
    for n, (c, kind) in enumerate(todo):
        _, _, shape, sign, second = CHUNKS[c]
        own = rest.pop(0)
        got = [rest.pop(0) for _ in range(3)]
        loads.append(pltpu.make_async_copy(ins[n], own, load.at[n]))
        start = sum(shape["widths"][:kind])
        out = outs[c].at[:, start : start + shape["widths"][kind]]
        sems = (send, recv, n * HOPS)
        if kind == 2:
            stages = sums_z(torus, second, own, got, out, sign, sems)
        else:
            wide = (rest.pop(0), rest.pop(0))
            pieces = rest.pop(0)
            wide[1][...] = jnp.zeros_like(wide[1])
            axes = ("x", "y") if kind == 0 else ("y", "x")
            stages = sums_xy(torus, *axes, own, got, wide, pieces, out, sign, sems, shape["r"], shape["rp"])
        stages[0] = functools.partial(lambda wait, go: (wait.wait(), go()), loads[-1], stages[0])
        stages_of[c].append(stages)
    for copy in loads:
        copy.start()
    torus.barrier()
    run_in_slots(stages_of)


def reduce_scatter(grads):
    todo = ranges()
    scratch = [
        pltpu.SemaphoreType.DMA((len(todo),)),
        pltpu.SemaphoreType.DMA((len(todo) * HOPS,)),
        pltpu.SemaphoreType.DMA((len(todo) * HOPS,)),
    ]
    for c, kind in todo:
        _, _, shape, _, second = CHUNKS[c]
        r, rp, width = shape["r"], shape["rp"], shape["widths"][kind]
        scratch.append(pltpu.VMEM(own_shape(shape, kind), BF16))
        if kind == 2:
            scratch.append(pltpu.VMEM((NZ - 1, NX, NY, rp, width), BF16))
            n2, n3 = (NX, NY) if second == "x" else (NY, NX)
            scratch.append(pltpu.VMEM((n2 - 1, n3, rp, width), BF16))
            scratch.append(pltpu.VMEM((n3 - 1, rp, width), BF16))
        else:
            n1, n2 = (NX, NY) if kind == 0 else (NY, NX)
            scratch.append(pltpu.VMEM((n1 - 1, n2, NZ * r, width), BF16))
            scratch.append(pltpu.VMEM((n2 - 1, NZ * r, width), BF16))
            scratch.append(pltpu.VMEM((NZ - 1, rp, width), BF16))
            scratch.append(pltpu.VMEM((NZ * r, width), F32))
            scratch.append(pltpu.VMEM((NZ, rp, width), F32))
            scratch.append(pltpu.VMEM((NZ, rp, width), BF16))
    return pl.pallas_call(
        reduce_kernel,
        out_shape=[jax.ShapeDtypeStruct((s["rp"], sum(s["widths"])), BF16) for _, _, s, _, _ in CHUNKS],
        in_specs=[pl.BlockSpec(memory_space=pl.ANY)] * len(todo),
        out_specs=[pl.BlockSpec(memory_space=pltpu.VMEM)] * len(CHUNKS),
        scratch_shapes=scratch,
        compiler_params=pltpu.CompilerParams(collective_id=0, has_side_effects=True, vmem_limit_bytes=67043328),
        name="reduce_scatter",
    )(*grads)


class GatherOver:
    def __init__(self, ring, place):
        self.ring, self.place = ring, place

    def shard(self, flow, hop):
        return self.ring.torus.shifted(self.ring.axis, -self.ring.signs[flow] * hop)

    def step(self, hop, src=None):
        for flow in (0, 1):
            if hop > self.ring.hops[flow]:
                continue
            place = self.place(self.shard(flow, hop))
            if hop:
                self.ring.copy(flow, hop, place, place).wait_recv()
            if hop < self.ring.hops[flow]:
                self.ring.start(flow, hop + 1, place if src is None else src, place)


def gathers_xy(torus, first, second, own, small, flat, place, sign, sems, r):
    me = torus.me
    send, recv, base = sems
    n1, n2 = torus.size[first], torus.size[second]
    rings = (
        Ring(torus, "z", sign, send, recv, base),
        Ring(torus, second, sign, send, recv, base + NZ - 1),
        Ring(torus, first, sign, send, recv, base + NZ + n2 - 2),
    )
    one = GatherOver(rings[0], lambda k: small.at[k])
    if first == "x":
        two = GatherOver(rings[1], lambda j: place.at[me["x"], j])
        three = GatherOver(rings[2], lambda i: place.at[i])
    else:
        two = GatherOver(rings[1], lambda i: place.at[i, me["y"]])
        three = GatherOver(rings[2], lambda j: place.at[:, j])

    def first_start():
        small[me["z"]] = own[...]
        one.step(0, src=own)

    def second_start():
        one.step(NZ // 2)
        for z in range(NZ):
            flat[z * r : (z + 1) * r, :] = small[z].astype(F32)[0:r, :]
        total(place.at[me["x"], me["y"]], [flat])
        two.step(0)

    def third_start():
        two.step(n2 // 2)
        three.step(0)

    def finish():
        three.step(n1 // 2)
        for ring in rings:
            ring.drain()

    stages = [first_start]
    stages += [functools.partial(one.step, h) for h in range(1, NZ // 2)]
    stages.append(second_start)
    stages += [functools.partial(two.step, h) for h in range(1, n2 // 2)]
    stages.append(third_start)
    stages += [functools.partial(three.step, h) for h in range(1, n1 // 2)]
    stages.append(finish)
    return stages


def gathers_z(torus, second, own, place, sign, sems):
    me = torus.me
    third = "y" if second == "x" else "x"
    send, recv, base = sems
    n2, n3 = torus.size[second], torus.size[third]
    rings = (
        Ring(torus, third, sign, send, recv, base),
        Ring(torus, second, sign, send, recv, base + n3 - 1),
        Ring(torus, "z", sign, send, recv, base + n3 + n2 - 2),
    )
    if third == "y":
        one = GatherOver(rings[0], lambda j: place.at[me["x"], j, me["z"]])
        two = GatherOver(rings[1], lambda i: place.at[i, :, me["z"]])
    else:
        one = GatherOver(rings[0], lambda i: place.at[i, me["y"], me["z"]])
        two = GatherOver(rings[1], lambda j: place.at[:, j, me["z"]])
    three = GatherOver(rings[2], lambda k: place.at[:, :, k])

    def first_start():
        place[me["x"], me["y"], me["z"]] = own[...]
        one.step(0, src=own)

    def second_start():
        one.step(n3 // 2)
        two.step(0)

    def third_start():
        two.step(n2 // 2)
        three.step(0)

    def finish():
        three.step(NZ // 2)
        for ring in rings:
            ring.drain()

    stages = [first_start]
    stages += [functools.partial(one.step, h) for h in range(1, n3 // 2)]
    stages.append(second_start)
    stages += [functools.partial(two.step, h) for h in range(1, n2 // 2)]
    stages.append(third_start)
    stages += [functools.partial(three.step, h) for h in range(1, NZ // 2)]
    stages.append(finish)
    return stages


def gather_kernel(*refs):
    todo = ranges()
    count = len(todo)
    ins, outs = refs[: len(CHUNKS)], refs[len(CHUNKS) : len(CHUNKS) + count]
    rest = list(refs[len(CHUNKS) + count :])
    store, send, recv = rest[:3]
    rest = rest[3:]
    torus = Torus()
    stages_of = [[] for _ in CHUNKS]
    stores = []
    for n, (c, kind) in enumerate(todo):
        _, _, shape, sign, second = CHUNKS[c]
        place = rest.pop(0)
        start = sum(shape["widths"][:kind])
        own = ins[c].at[:, start : start + shape["widths"][kind]]
        sems = (send, recv, n * HOPS)
        if kind == 2:
            stages = gathers_z(torus, second, own, place, sign, sems)
        else:
            axes = ("x", "y") if kind == 0 else ("y", "x")
            stages = gathers_xy(torus, *axes, own, rest.pop(0), rest.pop(0), place, sign, sems, shape["r"])
        stores.append(pltpu.make_async_copy(place, outs[n], store.at[n]))
        stages[-1] = functools.partial(lambda go, put: (go(), put.start()), stages[-1], stores[-1])
        stages_of[c].append(stages)
    torus.barrier()
    run_in_slots(stages_of)
    for copy in stores:
        copy.wait()


def all_gather(blocks):
    todo = ranges()
    scratch = [
        pltpu.SemaphoreType.DMA((len(todo),)),
        pltpu.SemaphoreType.DMA((len(todo) * HOPS,)),
        pltpu.SemaphoreType.DMA((len(todo) * HOPS,)),
    ]
    outs = []
    for c, kind in todo:
        shape = CHUNKS[c][2]
        scratch.append(pltpu.VMEM(own_shape(shape, kind), BF16))
        if kind != 2:
            scratch.append(pltpu.VMEM((NZ, shape["rp"], shape["widths"][kind]), BF16))
            scratch.append(pltpu.VMEM((NZ * shape["r"], shape["widths"][kind]), F32))
        outs.append(jax.ShapeDtypeStruct(own_shape(shape, kind), BF16))
    return pl.pallas_call(
        gather_kernel,
        out_shape=outs,
        in_specs=[pl.BlockSpec(memory_space=pltpu.VMEM)] * len(CHUNKS),
        out_specs=[pl.BlockSpec(memory_space=pl.ANY)] * len(todo),
        scratch_shapes=scratch,
        compiler_params=pltpu.CompilerParams(collective_id=1, has_side_effects=True, vmem_limit_bytes=67043328),
        name="all_gather",
    )(*blocks)


def unpack_kernel(r, widths, *refs):
    *ins, out, flat = refs
    per = len(ins) // 2
    layer = pl.program_id(0)
    for l in range(2):

        @pl.when(layer == l)
        def _():
            start = 0
            for kind, ref in enumerate(ins[l * per : (l + 1) * per]):
                width = widths[l][kind]
                if kind < 2:
                    out[0, :, start : start + width] = ref[0, 0]
                else:
                    for z in range(NZ):
                        flat[z * r : (z + 1) * r, :] = ref[0, 0, z].astype(F32)[0:r, :]
                    out[0, :, start : start + width] = flat[...].astype(BF16)
                start += width


def unpack(shapes, layers):
    r = shapes[0]["r"]
    columns = sum(shapes[0]["widths"])
    widths = [s["widths"] for s in shapes]
    specs = []
    for l in range(2):
        for kind in range(3):
            if not widths[l][kind]:
                continue
            if l == 0:
                at = lambda layer, p: jnp.where(layer == 0, p, NX * NY - 1)
            else:
                at = lambda layer, p: jnp.where(layer == 1, p, 0)
            if kind == 2:
                block = (1, 1, NZ, shapes[l]["rp"], widths[l][2])
                specs.append(pl.BlockSpec(block, lambda layer, p, at=at: (at(layer, p) // NY, at(layer, p) % NY, 0, 0, 0)))
            else:
                block = (1, 1, NZ * r, widths[l][kind])
                specs.append(pl.BlockSpec(block, lambda layer, p, at=at: (at(layer, p) // NY, at(layer, p) % NY, 0, 0)))
    return pl.pallas_call(
        functools.partial(unpack_kernel, r, widths),
        grid=(2, NX * NY),
        out_shape=jax.ShapeDtypeStruct((2, NX * NY * NZ * r, columns), BF16),
        in_specs=specs,
        out_specs=pl.BlockSpec((1, NZ * r, columns), lambda layer, p: (layer, p, 0)),
        scratch_shapes=[pltpu.VMEM((NZ * r, max(widths[0][2], 128)), F32)],
        name="unpack",
    )(*layers[0], *layers[1])


def dot(a, b, contract=((1,), (0,))):
    return lax.dot_general(a, b, (contract, ((), ())), preferred_element_type=F32)


def normed(h):
    wide = h.astype(F32)
    scale = lax.rsqrt(jnp.mean(wide**2, -1, keepdims=True) + 1e-6)
    return (wide * scale).astype(BF16), scale


def through(ct, gate, up, w_down):
    by_hidden = dot(ct, w_down, ((1,), (1,))).astype(BF16).astype(F32)
    sig = jax.nn.sigmoid(gate)
    silu = gate * sig
    by_gate = by_hidden * up * (sig * (1 + gate * (1 - sig)))
    return by_gate.astype(BF16), (by_hidden * silu).astype(BF16)


def local_gradients(x, dy, weights):
    w_gate, w_up, w_down = weights
    spread = (jnp.arange(D)[:, None] // 7 * 8 + jnp.arange(D)[:, None] % 7 == jnp.arange(D // 7 * 8)[None, :]).astype(BF16)

    def up_to_hidden(h, l):
        a, scale = normed(h)
        gate, up = dot(a, w_gate[l]), dot(a, w_up[l])
        return a, scale, gate, up, (jax.nn.silu(gate) * up).astype(BF16)

    a0, _, gate0, up0, hidden0 = up_to_hidden(x, 0)
    h1 = x + dot(hidden0, w_down[0]).astype(BF16)
    a1, scale1, gate1, up1, hidden1 = up_to_hidden(h1, 1)
    by_gate1, by_up1 = through(dy, gate1, up1, w_down[1])
    by_a = (dot(by_gate1, w_gate[1], ((1,), (1,))) + dot(by_up1, w_up[1], ((1,), (1,)))).astype(BF16).astype(F32)
    wide = h1.astype(F32)
    inner = jnp.mean(by_a * wide, -1, keepdims=True)
    by_h = dy + (by_a * scale1 - wide * (scale1**3 * inner)).astype(BF16)
    by_gate0, by_up0 = through(by_h, gate0, up0, w_down[0])
    grads = []
    for name, l, shape, _, _ in CHUNKS:
        widths = shape["widths"]
        if name == "w_down":
            hidden, ct = ((hidden0, by_h), (hidden1, dy))[l]
            g = dot(hidden, ct, ((0,), (0,))).astype(BF16)
            parts = [g[:, : widths[0]], g[:, widths[0] :]]
        else:
            a = (a0, a1)[l]
            by = ((by_gate0, by_up0), (by_gate1, by_up1))[l][name == "w_up"]
            g = dot(a, by[:, : widths[0] + widths[1]], ((0,), (0,))).astype(BF16)
            a_spread = dot(a, spread).astype(BF16)
            gz = dot(a_spread, by[:, widths[0] + widths[1] :], ((0,), (0,))).astype(BF16)
            parts = [g[:, : widths[0]], g[:, widths[0] :], gz]
        grads += [part.reshape(own_shape(shape, kind)) for kind, part in enumerate(parts)]
    return grads


def adamw(w, m, v, g):
    m = 0.9 * m + 0.1 * g
    v = 0.95 * v + 0.05 * g * g
    step = m * lax.rsqrt(v + 1e-8) + 0.1 * w
    return (w - 0.02 * step).astype(BF16), m, v


NAMES = ("w_gate", "w_up", "w_down")


def solution(mesh):
    def step(x, dy, *arrays):
        weights, ms, vs = (arrays[i : i + 3] for i in (0, 3, 6))
        sums = reduce_scatter(local_gradients(x[0], dy[0], weights))
        dp = lax.axis_index("dp")
        blocks, new_m, new_v = {}, {}, {}
        for (name, l, shape, _, _), g in zip(CHUNKS, sums, strict=True):
            n, r = NAMES.index(name), shape["r"]
            w = lax.dynamic_slice_in_dim(weights[n][l], dp * r, r, 0)
            w, m, v = adamw(w.astype(F32), ms[n][l], vs[n][l], g[:r].astype(F32))
            blocks[name, l] = jnp.pad(w, ((0, shape["rp"] - r), (0, 0)))
            new_m[name, l], new_v[name, l] = m, v
        gathered = list(all_gather([blocks[name, l] for name, l, *_ in CHUNKS]))
        layers = {}
        for name, l, shape, _, _ in CHUNKS:
            layers[name, l] = [gathered.pop(0) for width in shape["widths"] if width]
        shapes = {(name, l): shape for name, l, shape, _, _ in CHUNKS}
        new_w = [unpack([shapes[n, 0], shapes[n, 1]], [layers[n, 0], layers[n, 1]]) for n in NAMES]
        return (
            *new_w,
            *(jnp.stack([new_m[n, 0], new_m[n, 1]]) for n in NAMES),
            *(jnp.stack([new_v[n, 0], new_v[n, 1]]) for n in NAMES),
        )

    batch, whole, rows = P(("rep", "dp")), P(), P(None, "dp")
    return jax.shard_map(
        step,
        mesh=mesh,
        in_specs=(batch, batch, *[whole] * 3, *[rows] * 6),
        out_specs=(*[P("rep")] * 3, *[P("rep", "dp")] * 6),
        check_vma=False,
    )
```
